32 devices in a mesh: row: 4 (over y, x), col: 8 (over z, core).
Axes of the slice: x: 2, y: 2, z: 4, core: 2. Of those that a mesh axis runs over, the one named last changes fastest.
Arguments:
- gradient: bfloat16 [2304, 18432], P('row', 'col'), may hold values from -6 to 6
- left_basis: bfloat16 [2304, 2304], P('row'), may hold values from -0.125 to 0.125
- right_basis: bfloat16 [18432, 18432], P('col', 'row'), may hold values from -0.046875 to 0.046875
- first_moment: float32 [2304, 18432], P('col', 'row'), may hold values from -3 to 3
- second_moment: float32 [2304, 18432], P('col', 'row'), may hold values from 0.25 to 4
Outputs:
- update: bfloat16 [2304, 18432], P('row', 'col')
- first_new: float32 [2304, 18432], P('col', 'row')
- second_new: float32 [2304, 18432], P('col', 'row')
The draws below stay inside these ranges and needn't reach their ends.
All inputs are finite; a program needn't handle non-finite values.
Results may differ from the reference program's by a relative error of at most 0.018.
Values may be sent and summed in bfloat16 or wider, within the bound.
A program may use at most 128 MiB of HBM per device.

```python
import math
import jax
import jax.numpy as jnp
from jax import lax

M = 2304
N = 18432
N_ROW = 4
N_COL = 8


def levels(key, dims, cuts, low, top_value):
    gain = 1.0
    for axis_at, parts in cuts:
        draws = jax.random.uniform(jax.random.fold_in(jax.random.fold_in(key, 6), axis_at), (parts,), jnp.float32, low / len(cuts), top_value / len(cuts))
        gain = gain * jnp.repeat(jnp.exp(draws), dims[axis_at] // parts).reshape((-1,) + (1,) * (len(dims) - 1 - axis_at))
    return gain


def normal_values(own_key, extent, spread, reach, pieces=(), kind=jnp.bfloat16):
    result = jax.random.normal(own_key, extent, jnp.float32) * spread
    if len(pieces) > 0:
        result = levels(own_key, extent, pieces, -0.22, 0.18) * result
    return jnp.clip(result, min=-reach, max=reach).astype(kind)


def setup_inputs(seed: int = 0) -> dict:
    arg_keys = jax.random.split(jax.random.key(seed), 6)
    gradient = normal_values(arg_keys[0], (M, N), 1.0, 6.0, ((0, 4), (1, 8)))
    left_basis = normal_values(arg_keys[1], (M, M), M ** -0.5, 0.125, ((0, 4),))
    right_basis = normal_values(arg_keys[2], (N, N), N ** -0.5, 0.046875, ((0, 8), (1, 4)))
    first_moment = normal_values(arg_keys[3], (M, N), 0.5, 3.0, ((0, 8), (1, 4)), jnp.float32)
    second_moment = jnp.clip(jnp.exp(math.log(4.0) - 2.7725887 * jax.random.uniform(arg_keys[4], (M, N), jnp.float32) ** levels(arg_keys[4], (M, N), ((0, 8), (1, 4)), -0.2, 0.2)), 0.25, 4.0)
    return {"gradient": gradient, "left_basis": left_basis, "right_basis": right_basis, "first_moment": first_moment, "second_moment": second_moment}


beta_one = 0.9
beta_two = 0.95
epsilon = 1e-08
correct_one = 1.0 - 0.9 ** 10
correct_two = 1.0 - 0.95 ** 10

def rounded(values):
    narrow = lax.optimization_barrier(values.astype(jnp.bfloat16))
    return narrow.astype(jnp.float32)

def reference(gradient, left_basis, right_basis, first_moment, second_moment):
    precise = lax.Precision.HIGHEST
    grad_wide = gradient.astype(jnp.float32)
    left_wide = left_basis.astype(jnp.float32)
    right_wide = right_basis.astype(jnp.float32)
    row_block = M // N_ROW
    col_block = N // N_COL

    def left_part(running, block_index):
        offset = (block_index * row_block).astype(jnp.int32)
        basis_rows = lax.dynamic_slice_in_dim(left_wide, offset, row_block, 0)
        grad_rows = lax.dynamic_slice_in_dim(grad_wide, offset, row_block, 0)
        partial_value = lax.dot_general(basis_rows, grad_rows, (((0,), (0,)), ((), ())), precision=precise)
        return (running + rounded(partial_value), None)
    summed, _ = lax.scan(left_part, jnp.zeros((M, N), jnp.float32), jnp.arange(N_ROW, dtype=jnp.int32))
    rotated_left = rounded(summed)

    def right_part(running, block_index):
        offset = (block_index * col_block).astype(jnp.int32)
        left_cols = lax.dynamic_slice_in_dim(rotated_left, offset, col_block, 1)
        basis_rows = lax.dynamic_slice_in_dim(right_wide, offset, col_block, 0)
        partial_value = jnp.dot(left_cols, basis_rows, precision=precise)
        return (running + rounded(partial_value), None)
    summed, _ = lax.scan(right_part, jnp.zeros((M, N), jnp.float32), jnp.arange(N_COL, dtype=jnp.int32))
    rotated = rounded(summed)
    first_new = beta_one * first_moment + (1.0 - beta_one) * rotated
    second_new = beta_two * second_moment + (1.0 - beta_two) * rotated * rotated
    step_rot = rounded(first_new / correct_one / (jnp.sqrt(second_new / correct_two) + epsilon))

    def back_part(running, block_index):
        offset = (block_index * (N // N_ROW)).astype(jnp.int32)
        step_cols = lax.dynamic_slice_in_dim(step_rot, offset, N // N_ROW, 1)
        basis_cols = lax.dynamic_slice_in_dim(right_wide, offset, N // N_ROW, 1)
        partial_value = lax.dot_general(step_cols, basis_cols, (((1,), (1,)), ((), ())), precision=precise)
        return (running + rounded(partial_value), None)
    summed, _ = lax.scan(back_part, jnp.zeros((M, N), jnp.float32), jnp.arange(N_ROW, dtype=jnp.int32))
    back_rot = rounded(summed)
    update = jnp.dot(left_wide, back_rot, precision=precise).astype(jnp.bfloat16)
    return (update, first_new, second_new)
```

```python
import functools

import jax
import jax.numpy as jnp
from jax import lax
from jax.sharding import PartitionSpec as P

beta_one = 0.9
beta_two = 0.95
epsilon = 1e-08
correct_one = 1.0 - 0.9**10
correct_two = 1.0 - 0.95**10


def pick_chunks(rows):
    for count in (3, 2):
        if rows % (8 * count) == 0:
            return count
    return 1


def exchange(block_of, count):
    me = lax.axis_index("row")
    blocks = []
    for shift in range(1, count):
        pairs = [(i, (i + shift) % count) for i in range(count)]
        target = lax.rem(me + shift, count)
        blocks.append(lax.ppermute(block_of(target), "row", pairs))
    return blocks


def scatter_sum(part, count):
    me = lax.axis_index("row")
    size = part.shape[0] // count

    def block_of(index):
        return lax.dynamic_slice_in_dim(part, index * size, size, 0)

    total = block_of(me).astype(jnp.float32)
    for block in exchange(block_of, count):
        total = total + block.astype(jnp.float32)
    return total.astype(jnp.bfloat16)


def gather_rows(own, count):
    me = lax.axis_index("row")
    size = own.shape[0]
    whole = jnp.zeros((size * count, own.shape[1]), own.dtype)
    whole = lax.dynamic_update_slice_in_dim(whole, own, me * size, 0)
    for shift, block in enumerate(exchange(lambda _: own, count), 1):
        origin = lax.rem(me + count - shift, count)
        whole = lax.dynamic_update_slice_in_dim(whole, block, origin * size, 0)
    return whole


def per_device(n_row, n_col, gradient, left_basis, right_basis, first_moment, second_moment):
    own_rows, _ = first_moment.shape
    chunks = pick_chunks(own_rows)
    step = own_rows // chunks
    width = gradient.shape[1]
    left_part = lax.dot_general(
        left_basis, gradient, (((0,), (0,)), ((), ())), preferred_element_type=jnp.float32
    ).astype(jnp.bfloat16)
    left_part = left_part.reshape(n_col, chunks, step, width)
    firsts, seconds, backs = [], [], []
    for k in range(chunks):
        piece = left_part[:, k].reshape(n_col * step, width)
        rotated_left = gather_rows(scatter_sum(piece, n_row), n_row)
        rotated = lax.psum_scatter(
            jnp.dot(rotated_left, right_basis, preferred_element_type=jnp.float32).astype(
                jnp.bfloat16
            ),
            "col",
            scatter_dimension=0,
            tiled=True,
        )
        wide = rotated.astype(jnp.float32)
        rows = slice(k * step, (k + 1) * step)
        first_new = beta_one * first_moment[rows] + (1.0 - beta_one) * wide
        second_new = beta_two * second_moment[rows] + (1.0 - beta_two) * wide * wide
        step_rot = (
            first_new / correct_one / (jnp.sqrt(second_new / correct_two) + epsilon)
        ).astype(jnp.bfloat16)
        firsts.append(first_new)
        seconds.append(second_new)
        back_part = lax.dot_general(
            lax.all_gather(step_rot, "col", axis=0, tiled=True),
            right_basis,
            (((1,), (1,)), ((), ())),
            preferred_element_type=jnp.float32,
        ).astype(jnp.bfloat16)
        back_rot = gather_rows(scatter_sum(back_part, n_row), n_row)
        backs.append(back_rot.reshape(n_col, step, width))
    back_rot = jnp.stack(backs, axis=1).reshape(n_col * own_rows, width)
    update = jnp.dot(left_basis, back_rot, preferred_element_type=jnp.float32).astype(jnp.bfloat16)
    return (update, jnp.concatenate(firsts, 0), jnp.concatenate(seconds, 0))


def solution(mesh):
    in_specs = (P("row", "col"), P("row", None), P("col", "row"), P("col", "row"), P("col", "row"))
    out_specs = (P("row", "col"), P("col", "row"), P("col", "row"))
    return jax.shard_map(
        functools.partial(per_device, mesh.shape["row"], mesh.shape["col"]),
        mesh=mesh, in_specs=in_specs, out_specs=out_specs, check_vma=False
    )
```
